128 devices in a mesh: ty: 8 (over x, core), tx: 16 (over y, z).
Axes of the slice: x: 4, y: 4, z: 4, core: 2. Of those that a mesh axis runs over, the one named last changes fastest.
Arguments:
- measured: float32 [8, 16, 32, 128, 128], P('ty', 'tx'), may hold values from 0 to 4
- positions: int32 [8, 16, 32, 2], P('ty', 'tx'), may hold values from 0 to 511, as said below
- owners: int32 [8, 16, 32], P('ty', 'tx'), may hold values from 0 to 127, as said below
- counts: int32 [8, 16], P('ty', 'tx'), may hold values from 16 to 32, as said below
- object_field: float32 [2, 4096, 8192], P(None, 'ty', 'tx'), may hold values from -4 to 4
- probe_field: float32 [2, 128, 128], replicated, may hold values from -6 to 6
Outputs:
- new_object: float32 [2, 4096, 8192], P(None, 'ty', 'tx')
- new_probe: float32 [2, 128, 128], replicated
The draws below stay inside these ranges and needn't reach their ends.
Inputs may be any that keep to these rules, and one draw needn't show every extreme that they name: `positions`: for a live slot the entry is a cell of the owner's tile: row below 512, column below 512; other slots hold arbitrary cells of a tile. The owner of a live slot is the holding device's own tile or one of the up to eight tiles beside it (diagonals included). From one device at most 2 live slots go to any one other tile, and in every draw some tile receives exactly 2 from each of its eight neighbours. Slots that are not live hold arbitrary owners. `counts`: some device is full (32 live slots) in every draw.
All inputs are finite; a program needn't handle non-finite values.
Results may differ from the reference program's by a relative error of at most 0.0003.
Values sent between devices are 32-bit elements; how exact they have to be, the bound alone decides.
A program may use at most 128 MiB of HBM per device.

```python
import jax
import jax.numpy as jnp
from jax import lax

M = 128
TH = 512
TW = 512
SLOTS = 32
MOVE = 2
NYC = 4096
NXC = 8192
N_TY = 8
N_TX = 16


def tile_layout(key):
    base = jax.random.fold_in(key, 7)
    keys_all = jax.random.split(base, 10)
    devices = N_TY * N_TX
    dev_ids = jnp.arange(devices, dtype=jnp.int32)
    dev_row = (dev_ids // N_TX)[:, None]
    dev_col = (dev_ids % N_TX)[:, None]
    step_rows = jnp.array([-1, -1, -1, 0, 0, 1, 1, 1], dtype=jnp.int32)
    step_cols = jnp.array([-1, 0, 1, -1, 1, -1, 0, 1], dtype=jnp.int32)
    dest_row = dev_row + step_rows[None, :]
    dest_col = dev_col + step_cols[None, :]
    inside = (dest_row >= 0) & (dest_row < N_TY) & (dest_col >= 0) & (dest_col < N_TX)
    hot_row = jax.random.randint(keys_all[0], (), 1, N_TY - 1)
    hot_col = jax.random.randint(keys_all[1], (), 1, N_TX - 1)
    is_hot = (dest_row == hot_row) & (dest_col == hot_col)
    movers = jax.random.randint(keys_all[2], (devices, 8), 0, MOVE + 1)
    movers = jnp.where(is_hot, MOVE, movers) * inside.astype(jnp.int32)
    slot_counts = jax.random.randint(keys_all[3], (devices,), 8 * MOVE, SLOTS + 1)
    fullest = jax.random.randint(keys_all[4], (), 0, devices)
    slot_counts = jnp.where(dev_ids == fullest, SLOTS, slot_counts)
    slot_ids = jnp.arange(SLOTS, dtype=jnp.int32)[None, :]
    scores = jax.random.randint(keys_all[5], (devices, SLOTS), 0, 1 << 16) * SLOTS + slot_ids
    scores = jnp.where(slot_ids < slot_counts[:, None], scores, scores + (1 << 16) * SLOTS)
    ranking = jnp.argsort(jnp.argsort(scores, axis=1), axis=1).astype(jnp.int32)
    bounds = jnp.cumsum(movers, axis=1)
    category = jnp.sum((ranking[:, :, None] >= bounds[:, None, :]).astype(jnp.int32), axis=2)
    moving = category < 8
    capped = jnp.minimum(category, 7)
    row_step = jnp.where(moving, step_rows[capped], 0)
    col_step = jnp.where(moving, step_cols[capped], 0)
    near_row = jax.random.randint(keys_all[6], (devices, SLOTS), 0, M // 2)
    near_col = jax.random.randint(keys_all[7], (devices, SLOTS), 0, M // 2)
    any_row = jax.random.randint(keys_all[8], (devices, SLOTS), 0, TH)
    any_col = jax.random.randint(keys_all[9], (devices, SLOTS), 0, TW)
    pos_row = jnp.where(row_step == -1, TH - 1 - near_row, jnp.where(row_step == 1, near_row, any_row))
    pos_col = jnp.where(col_step == -1, TW - 1 - near_col, jnp.where(col_step == 1, near_col, any_col))
    live_slots = slot_ids < slot_counts[:, None]
    stray_owner = jax.random.randint(jax.random.fold_in(base, 11), (devices, SLOTS), 0, devices)
    owner_ids = jnp.where(live_slots, (dev_row + row_step) * N_TX + dev_col + col_step, stray_owner)
    position_table = jnp.stack([pos_row, pos_col], axis=-1).reshape(N_TY, N_TX, SLOTS, 2).astype(jnp.int32)
    return (position_table, owner_ids.reshape(N_TY, N_TX, SLOTS).astype(jnp.int32), slot_counts.reshape(N_TY, N_TX).astype(jnp.int32))


def draw_positions(key, part):
    return tile_layout(key)[0]


def draw_owners(key, part):
    return tile_layout(key)[1]


def draw_counts(key, part):
    return tile_layout(key)[2]


def steps_of(key, dims, shards, least, largest):
    def one(dim, parts):
        steps = jax.random.uniform(jax.random.fold_in(jax.random.fold_in(key, 6), dim), (parts,), jnp.float32, least / len(shards), largest / len(shards))
        return jnp.repeat(jnp.exp(steps), dims[dim] // parts).reshape((-1,) + (1,) * (len(dims) - dim - 1))

    level = one(*shards[0])
    for cut in shards[1:]:
        level = level * one(*cut)
    return level


def scatter_about(stream_key, dims, deviation, reach, cuts=(), kind=jnp.bfloat16):
    values = deviation * jax.random.normal(stream_key, dims, jnp.float32)
    if cuts:
        values = values * steps_of(stream_key, dims, cuts, -0.22, 0.18)
    return jnp.clip(values, -reach, reach).astype(kind)


def setup_inputs(seed: int = 0) -> dict:
    keys = jax.random.split(jax.random.key(seed), 7)
    measured = jnp.clip(4.0 * jax.random.uniform(keys[0], (N_TY, N_TX, SLOTS, M, M), jnp.float32) ** steps_of(keys[0], (N_TY, N_TX, SLOTS, M, M), ((0, 8), (1, 16)), -0.2, 0.2), 0.0, 4.0)
    positions = draw_positions(jax.random.fold_in(keys[6], 71), 0)
    owners = draw_owners(jax.random.fold_in(keys[6], 71), 0)
    counts = draw_counts(jax.random.fold_in(keys[6], 71), 0)
    object_field = scatter_about(keys[4], (2, NYC, NXC), 0.7, 4.0, ((1, 8), (2, 16)), jnp.float32)
    probe_field = scatter_about(keys[5], (2, M, M), 1.0, 6.0, (), jnp.float32)
    return {"measured": measured, "positions": positions, "owners": owners, "counts": counts, "object_field": object_field, "probe_field": probe_field}


offset_level = 1.0
floor_level = 1.0
tiny_level = 1e-6


def pattern_terms(probe_field, patches, measured_block, live_mask):
    probe_real = probe_field[0]
    probe_imag = probe_field[1]
    patch_real = patches[:, 0]
    patch_imag = patches[:, 1]
    exit_real = probe_real * patch_real - probe_imag * patch_imag
    exit_imag = probe_real * patch_imag + probe_imag * patch_real
    farfield = jnp.fft.fft2(lax.complex(exit_real, exit_imag), norm="ortho")
    far_real = jnp.real(farfield)
    far_imag = jnp.imag(farfield)
    power = far_real * far_real + far_imag * far_imag
    ratio = 1.0 - measured_block / (power + offset_level)
    backward = jnp.fft.ifft2(lax.complex(far_real * ratio, far_imag * ratio), norm="ortho")
    chi_real = jnp.real(backward) * live_mask[:, None, None]
    chi_imag = jnp.imag(backward) * live_mask[:, None, None]
    object_real = probe_real * chi_real + probe_imag * chi_imag
    object_imag = probe_real * chi_imag - probe_imag * chi_real
    lighting = (probe_real * probe_real + probe_imag * probe_imag)[None] * live_mask[:, None, None]
    spread = jnp.stack([object_real, object_imag, lighting], axis=1)
    grad_real = jnp.sum(patch_real * chi_real + patch_imag * chi_imag, axis=0)
    grad_imag = jnp.sum(patch_real * chi_imag - patch_imag * chi_real, axis=0)
    weight = jnp.sum((patch_real * patch_real + patch_imag * patch_imag) * live_mask[:, None, None], axis=0)
    return spread, grad_real, grad_imag, weight


def add_patches(accumulated, spread, start_rows, start_cols):
    zero_index = jnp.zeros((), jnp.int32)

    def add_one(patch_id, current):
        row_start = start_rows[patch_id]
        col_start = start_cols[patch_id]
        window = lax.dynamic_slice(current, (zero_index, row_start, col_start), spread.shape[1:])
        return lax.dynamic_update_slice(current, window + spread[patch_id], (zero_index, row_start, col_start))

    return lax.fori_loop(0, spread.shape[0], add_one, accumulated)


def reference(measured, positions, owners, counts, object_field, probe_field):
    rim_width = M // 2
    tile_rows = object_field.shape[1] // N_TY
    tile_cols = object_field.shape[2] // N_TX
    padded = jnp.pad(object_field, ((0, 0), (rim_width, rim_width), (rim_width, rim_width)))
    devices = N_TY * N_TX
    flat_measured = measured.reshape(devices, SLOTS, M, M)
    flat_positions = positions.reshape(devices, SLOTS, 2).astype(jnp.int32)
    flat_owners = owners.reshape(devices, SLOTS).astype(jnp.int32)
    flat_counts = counts.reshape(devices).astype(jnp.int32)
    slot_ids = jnp.arange(SLOTS, dtype=jnp.int32)
    zero_index = jnp.zeros((), jnp.int32)

    def per_device(state_carry, inputs_now):
        accumulated, grad_real, grad_imag, weight = state_carry
        measured_now, positions_now, owners_now, count_now = inputs_now
        live_mask = (slot_ids < count_now).astype(jnp.float32)
        start_rows = ((owners_now // N_TX) * tile_rows + positions_now[:, 0]).astype(jnp.int32)
        start_cols = ((owners_now % N_TX) * tile_cols + positions_now[:, 1]).astype(jnp.int32)
        patches = jax.vmap(lambda row_start, col_start: lax.dynamic_slice(padded, (zero_index, row_start, col_start), (2, M, M)))(start_rows, start_cols)
        spread, part_real, part_imag, part_weight = pattern_terms(probe_field, patches, measured_now, live_mask)
        accumulated = add_patches(accumulated, spread, start_rows, start_cols)
        return (accumulated, grad_real + part_real, grad_imag + part_imag, weight + part_weight), None

    start_state = (jnp.zeros((3, padded.shape[1], padded.shape[2]), jnp.float32), jnp.zeros((M, M), jnp.float32), jnp.zeros((M, M), jnp.float32), jnp.zeros((M, M), jnp.float32))
    final_state, _ = lax.scan(per_device, start_state, (flat_measured, flat_positions, flat_owners, flat_counts))
    accumulated, grad_real, grad_imag, weight = final_state
    interior = accumulated[:, rim_width:rim_width + object_field.shape[1], rim_width:rim_width + object_field.shape[2]]
    new_object = object_field - interior[:2] / (interior[2] + floor_level)
    new_probe = probe_field - jnp.stack([grad_real, grad_imag]) / (weight + tiny_level)
    return new_object, new_probe
```

```python
import functools

import jax
import jax.numpy as jnp
import numpy as np
from jax import lax
from jax.experimental import pallas as pl
from jax.experimental.pallas import tpu as pltpu
from jax.sharding import PartitionSpec as P

M = 128
MOVE = 2
RIM = M // 2
LANES = 128
BATCH = 4

offset_level = 1.0
floor_level = 1.0
tiny_level = 1e-06

MESH_ID = pl.DeviceIdType.MESH
DIRECTIONS = [(-1, -1), (-1, 0), (-1, 1), (0, -1), (0, 1), (1, -1), (1, 0), (1, 1)]
CORNERS = [(-1, -1), (-1, 1), (1, -1), (1, 1)]

F32 = jnp.float32
BF16 = jnp.bfloat16
I32 = jnp.int32


def in_vmem():
    return pl.BlockSpec(memory_space=pltpu.VMEM)


def in_smem():
    return pl.BlockSpec(memory_space=pltpu.SMEM)


def anywhere():
    return pl.BlockSpec(memory_space=pl.ANY)


def dft_tables():
    phase = (np.outer(np.arange(M), np.arange(M)) % M) * (2.0 * np.pi / M)
    c, s = np.cos(phase) / np.sqrt(M), -np.sin(phase) / np.sqrt(M)
    forward = np.block([[c, s], [-s, c]])
    tables = []
    for table in (forward, forward.T):
        high = table.astype(BF16)
        tables += [high, (table - high.astype(np.float64)).astype(BF16)]
    return tables


def lane_ids(rows):
    return lax.broadcasted_iota(I32, (rows, LANES), 1)


def neighbour(down, right):
    ty, tx = lax.axis_index("ty"), lax.axis_index("tx")
    n_ty, n_tx = lax.axis_size("ty"), lax.axis_size("tx")
    return lax.rem(ty + (down + n_ty), n_ty), lax.rem(tx + (right + n_tx), n_tx)


def is_inside(down, right):
    ty, tx = lax.axis_index("ty"), lax.axis_index("tx")
    row, col = ty + down, tx + right
    return (row >= 0) & (row < lax.axis_size("ty")) & (col >= 0) & (col < lax.axis_size("tx"))


def pack_left(first, second, rows):
    return jnp.where(lane_ids(rows) >= RIM, first, pltpu.roll(second, RIM, 1))


def pack_right(first, second, rows):
    return jnp.where(lane_ids(rows) < RIM, first, pltpu.roll(second, RIM, 1))


def spread_kernel(
    owners_ref,
    positions_ref,
    counts_ref,
    measured_ref,
    object_ref,
    pattern_out,
    tag_out,
    side_out,
    row_out,
    corner_out,
    pattern_pack,
    tag_pack,
    side_pack,
    send_sem,
    recv_sem,
):
    slots = measured_ref.shape[0]
    rows, cols = object_ref.shape[1:]
    n_tx = lax.axis_size("tx")
    ty, tx = lax.axis_index("ty"), lax.axis_index("tx")

    barrier = pltpu.get_barrier_semaphore()
    for down, right in DIRECTIONS:
        pl.semaphore_signal(barrier, inc=1, device_id=neighbour(down, right), device_id_type=MESH_ID)
    edge = pl.ds(cols - LANES, LANES)
    side_pack[0] = pack_left(object_ref[0, :, edge], object_ref[1, :, edge], rows)
    side_pack[1] = pack_right(object_ref[0, :, :LANES], object_ref[1, :, :LANES], rows)
    pl.semaphore_wait(barrier, len(DIRECTIONS))

    copies = []

    def send(source, target, down, right):
        slot = len(copies)
        copy = pltpu.make_async_remote_copy(
            src_ref=source,
            dst_ref=target,
            send_sem=send_sem.at[slot],
            recv_sem=recv_sem.at[slot],
            device_id=neighbour(down, right),
            device_id_type=MESH_ID,
        )
        copy.start()
        copies.append(copy)

    send(side_pack.at[0], side_out.at[0], 0, 1)
    send(side_pack.at[1], side_out.at[1], 0, -1)
    send(object_ref.at[:, pl.ds(rows - RIM, RIM), :], row_out.at[0], 1, 0)
    send(object_ref.at[:, pl.ds(0, RIM), :], row_out.at[1], -1, 0)
    for corner, (down, right) in enumerate(CORNERS):
        source = side_pack.at[0 if right == 1 else 1, pl.ds(0 if down == -1 else rows - RIM, RIM), :]
        send(source, corner_out.at[corner], down, right)

    count = counts_ref[0, 0]
    lane = lane_ids(1)
    for way, (down, right) in enumerate(DIRECTIONS):
        target = jnp.where(is_inside(down, right), (ty + down) * n_tx + (tx + right), -1)
        found, first, second = jnp.int32(0), jnp.int32(0), jnp.int32(0)
        for slot in range(slots):
            hit = (owners_ref[0, 0, slot] == target) & (slot < count)
            first = jnp.where(hit & (found == 0), slot, first)
            second = jnp.where(hit & (found == 1), slot, second)
            found = found + hit.astype(I32)
        tag = jnp.zeros((1, LANES), I32)
        for index, chosen in enumerate((first, second)):
            pattern_pack[way, index] = measured_ref[chosen]
            valid = (found > index).astype(I32)
            tag = jnp.where(lane == 3 * index, valid, tag)
            tag = jnp.where(lane == 3 * index + 1, positions_ref[0, 0, chosen, 0], tag)
            tag = jnp.where(lane == 3 * index + 2, positions_ref[0, 0, chosen, 1], tag)
        tag_pack[way] = tag
    for way, (down, right) in enumerate(DIRECTIONS):
        send(tag_pack.at[way], tag_out.at[way], down, right)
        send(pattern_pack.at[way], pattern_out.at[way], down, right)
    for copy in copies:
        copy.wait()


def spread(owners, positions, counts, measured, object_field):
    rows, cols = object_field.shape[1:]
    ways = len(DIRECTIONS)
    copies = 4 + len(CORNERS) + 2 * ways
    return pl.pallas_call(
        spread_kernel,
        out_shape=(
            jax.ShapeDtypeStruct((ways, MOVE, M, M), F32),
            jax.ShapeDtypeStruct((ways, 1, LANES), I32),
            jax.ShapeDtypeStruct((2, rows, LANES), F32),
            jax.ShapeDtypeStruct((2, 2, RIM, cols), F32),
            jax.ShapeDtypeStruct((len(CORNERS), RIM, LANES), F32),
        ),
        in_specs=[in_smem(), in_smem(), in_smem(), in_vmem(), in_vmem()],
        out_specs=(anywhere(),) * 5,
        scratch_shapes=[
            pltpu.VMEM((ways, MOVE, M, M), F32),
            pltpu.VMEM((ways, 1, LANES), I32),
            pltpu.VMEM((2, rows, LANES), F32),
            pltpu.SemaphoreType.DMA((copies,)),
            pltpu.SemaphoreType.DMA((copies,)),
        ],
        compiler_params=pltpu.CompilerParams(
            collective_id=0, has_side_effects=True, vmem_limit_bytes=16 << 20
        ),
        name="spread",
    )(owners, positions, counts, measured, object_field)


PADDED_BLOCKS = 2


def split(value):
    high = value.astype(BF16)
    return high, (value - high.astype(F32)).astype(BF16)


def dot(a, b):
    return jnp.dot(a, b, preferred_element_type=F32)


def patterns_kernel(
    owners_ref,
    positions_ref,
    counts_ref,
    tag_ref,
    measured_ref,
    arrived_ref,
    object_ref,
    side_ref,
    row_ref,
    corner_ref,
    probe_ref,
    uh_ref,
    ul_ref,
    vh_ref,
    vl_ref,
    sums_ref,
    left_ref,
    right_ref,
    probe_sums_ref,
    field,
    shifted,
    turned_sums,
    data,
    window,
    framed,
    xh,
    xl,
    yh,
    yl,
    row_list,
    col_list,
    data_list,
    copy_sem,
):
    slots = owners_ref.shape[2]
    rows, cols = object_ref.shape[1:]
    blocks = cols // LANES
    n_tx = lax.axis_size("tx")
    ty, tx = lax.axis_index("ty"), lax.axis_index("tx")
    self_index = ty * n_tx + tx
    moved = 2 * len(DIRECTIONS)

    own_copy = pltpu.make_async_copy(measured_ref, data.at[pl.ds(0, slots)], copy_sem.at[0])
    own_copy.start()
    moved_copy = pltpu.make_async_copy(arrived_ref, data.at[pl.ds(slots, moved)], copy_sem.at[1])
    moved_copy.start()

    for part in range(2):
        for block in range(blocks):
            field[part, 1 + block, RIM : RIM + rows, :] = object_ref[part, :, block * LANES : (block + 1) * LANES]
            field[part, 1 + block, :RIM, :] = jnp.where(
                is_inside(-1, 0), row_ref[0, part, :, block * LANES : (block + 1) * LANES], 0.0
            )
            field[part, 1 + block, RIM + rows :, :] = jnp.where(
                is_inside(1, 0), row_ref[1, part, :, block * LANES : (block + 1) * LANES], 0.0
            )

    def unpacked(part, value):
        return value if part == 0 else pltpu.roll(value, RIM, 1)

    for part in range(2):
        field[part, 0, RIM : RIM + rows, :] = jnp.where(is_inside(0, -1), unpacked(part, side_ref[0]), 0.0)
        field[part, 1 + blocks, RIM : RIM + rows, :] = jnp.where(is_inside(0, 1), unpacked(part, side_ref[1]), 0.0)
        for corner, (down, right) in enumerate(CORNERS):
            here = pl.ds(0, RIM) if down == 1 else pl.ds(RIM + rows, RIM)
            field[part, 0 if right == 1 else 1 + blocks, here, :] = jnp.where(
                is_inside(-down, -right), unpacked(part, corner_ref[corner]), 0.0
            )

    for turn in range(8):
        for part in range(2):
            value = probe_ref[part]
            shifted[turn, part] = pltpu.roll(value, turn, 0) if turn else value
    sums_ref[...] = jnp.zeros(sums_ref.shape, F32)
    turned_sums[...] = jnp.zeros(turned_sums.shape, F32)

    count = counts_ref[0, 0]

    def own(slot, total):
        row_list[total] = positions_ref[0, 0, slot, 0]
        col_list[total] = positions_ref[0, 0, slot, 1]
        data_list[total] = slot
        return total + ((owners_ref[0, 0, slot] == self_index) & (slot < count)).astype(I32)

    total = lax.fori_loop(0, slots, own, jnp.int32(0))
    for way in range(len(DIRECTIONS)):
        for index in range(MOVE):
            row_list[total] = tag_ref[way, 0, 3 * index + 1]
            col_list[total] = tag_ref[way, 0, 3 * index + 2]
            data_list[total] = slots + way * MOVE + index
            total = total + tag_ref[way, 0, 3 * index]
    for index in range(BATCH):
        row_list[total + index] = 0
        col_list[total + index] = 0
        data_list[total + index] = 0

    own_copy.wait()
    moved_copy.wait()
    lane_of_frame = lane_ids(M)
    lane_of_window = lane_ids(M + 8)
    row_of_tile = lax.broadcasted_iota(I32, (8, LANES), 0)

    def place(step, index):
        number = step * BATCH + index
        row, col = row_list[number], col_list[number] + RIM
        turn, lane = row & 7, col & (LANES - 1)
        return number, pl.multiple_of(row - turn, 8), lax.shift_right_logical(col, 7), turn, lane

    def one_batch(step, _):
        for index in range(BATCH):
            _, row, block, turn, lane = place(step, index)
            later = lane_of_window >= lane
            kept = row_of_tile >= turn
            parts = []
            for part in range(2):
                here = field[part, block, pl.ds(row, M + 8), :]
                beside = field[part, block + 1, pl.ds(row, M + 8), :]
                value = jnp.where(later, here, beside)
                value = jnp.concatenate([jnp.where(kept, value[:8], value[M:]), value[8:M]], axis=0)
                window[index, part] = value
                parts.append(value)
            wr, wi = parts
            pr = pltpu.roll(shifted[turn, 0], lane, 1)
            pi = pltpu.roll(shifted[turn, 1], lane, 1)
            framed[index, 0] = pr
            framed[index, 1] = pi
            at = pl.ds(index * M, M)
            for part, value in enumerate((pr * wr - pi * wi, pr * wi + pi * wr)):
                xh[at, part * M : (part + 1) * M], xl[at, part * M : (part + 1) * M] = split(value)

        def right_product(high, low):
            a = xh[...]
            return dot(a, high[...]) + dot(xl[...], high[...]) + dot(a, low[...])

        def to_pairs(value):
            for index in range(BATCH):
                for part in range(2):
                    piece = value[index * M : (index + 1) * M, part * M : (part + 1) * M]
                    to = (index // 2, pl.ds(part * M, M), pl.ds((index % 2) * M, M))
                    yh[to], yl[to] = split(piece)

        def left_product(pair, high, low):
            return dot(high[...], yh[pair]) + dot(high[...], yl[pair]) + dot(low[...], yh[pair])

        to_pairs(right_product(uh_ref, ul_ref))
        for pair in range(BATCH // 2):
            far = left_product(pair, vh_ref, vl_ref)
            for half in range(2):
                index = 2 * pair + half
                fr = far[:M, half * M : (half + 1) * M]
                fi = far[M:, half * M : (half + 1) * M]
                number = step * BATCH + index
                ratio = 1.0 - data[data_list[number]] / (fr * fr + fi * fi + offset_level)
                at = pl.ds(index * M, M)
                for part, value in enumerate((fr * ratio, fi * ratio)):
                    xh[at, part * M : (part + 1) * M], xl[at, part * M : (part + 1) * M] = split(value)
        to_pairs(right_product(vh_ref, vl_ref))
        for pair in range(BATCH // 2):
            back = left_product(pair, uh_ref, ul_ref)
            for half in range(2):
                index = 2 * pair + half
                number, row, block, turn, lane = place(step, index)
                live = (number < total).astype(F32)
                cr = back[:M, half * M : (half + 1) * M] * live
                ci = back[M:, half * M : (half + 1) * M] * live
                wr, wi = window[index, 0], window[index, 1]
                pr, pi = framed[index, 0], framed[index, 1]
                back_lanes = (LANES - lane) & (LANES - 1)
                terms = (wr * cr + wi * ci, wr * ci - wi * cr, (wr * wr + wi * wi) * live)
                for kind, term in enumerate(terms):
                    turned_sums[turn, kind] += pltpu.roll(term, back_lanes, 1)
                later = lane_of_frame >= lane
                kept = row_of_tile >= turn
                terms = (pr * cr + pi * ci, pr * ci - pi * cr, (pr * pr + pi * pi) * live)
                for kind, term in enumerate(terms):
                    for beside in range(2):
                        piece = jnp.where(later, 0.0, term) if beside else jnp.where(later, term, 0.0)
                        top = piece[:8]
                        sums_ref[kind, block + beside, pl.ds(row + 8, M - 8), :] += piece[8:]
                        sums_ref[kind, block + beside, pl.ds(row, 8), :] += jnp.where(kept, top, 0.0)
                        sums_ref[kind, block + beside, pl.ds(row + M, 8), :] += jnp.where(kept, 0.0, top)
        return _

    lax.fori_loop(0, lax.div(total + (BATCH - 1), BATCH), one_batch, 0)

    for kind in range(3):
        total_of_kind = turned_sums[0, kind]
        for turn in range(1, 8):
            total_of_kind = total_of_kind + pltpu.roll(turned_sums[turn, kind], M - turn, 0)
        probe_sums_ref[kind] = total_of_kind

    half = rows // 2
    for pack, out, block in ((pack_left, left_ref, 0), (pack_right, right_ref, 1 + blocks)):
        def rim(kind, start, length):
            return sums_ref[kind, block, start : start + length, :]

        out[:rows, :] = pack(rim(0, RIM, rows), rim(1, RIM, rows), rows)
        out[rows : rows + half, :] = pack(rim(2, RIM, half), rim(2, RIM + half, half), half)
        at = rows + half
        for start in (0, RIM + rows):
            out[at : at + RIM, :] = pack(rim(0, start, RIM), rim(1, start, RIM), RIM)
            out[at + RIM : at + RIM + RIM // 2, :] = pack(
                rim(2, start, RIM // 2), rim(2, start + RIM // 2, RIM // 2), RIM // 2
            )
            at += RIM + RIM // 2


def patterns(owners, positions, counts, tags, measured, arrived, object_field, sides, edges, corners, probe):
    slots = measured.shape[0]
    rows, cols = object_field.shape[1:]
    blocks = cols // LANES + PADDED_BLOCKS
    moved = 2 * len(DIRECTIONS)
    packed = rows + rows // 2 + 3 * RIM
    entries = slots + moved + BATCH
    return pl.pallas_call(
        patterns_kernel,
        out_shape=(
            jax.ShapeDtypeStruct((3, blocks, rows + 2 * RIM, LANES), F32),
            jax.ShapeDtypeStruct((packed, LANES), F32),
            jax.ShapeDtypeStruct((packed, LANES), F32),
            jax.ShapeDtypeStruct((3, M, M), F32),
        ),
        in_specs=[in_smem()] * 4 + [anywhere()] * 2 + [in_vmem()] * 9,
        out_specs=(in_vmem(),) * 4,
        scratch_shapes=[
            pltpu.VMEM((2, blocks, rows + 2 * RIM, LANES), F32),
            pltpu.VMEM((8, 2, M, M), F32),
            pltpu.VMEM((8, 3, M, M), F32),
            pltpu.VMEM((slots + moved, M, M), F32),
            pltpu.VMEM((BATCH, 2, M, M), F32),
            pltpu.VMEM((BATCH, 2, M, M), F32),
            pltpu.VMEM((BATCH * M, 2 * M), BF16),
            pltpu.VMEM((BATCH * M, 2 * M), BF16),
            pltpu.VMEM((BATCH // 2, 2 * M, 2 * M), BF16),
            pltpu.VMEM((BATCH // 2, 2 * M, 2 * M), BF16),
            pltpu.SMEM((entries,), I32),
            pltpu.SMEM((entries,), I32),
            pltpu.SMEM((entries,), I32),
            pltpu.SemaphoreType.DMA((2,)),
        ],
        compiler_params=pltpu.CompilerParams(vmem_limit_bytes=40 << 20),
        name="patterns",
    )(
        owners, positions, counts, tags, measured, arrived.reshape(moved, M, M), object_field,
        sides, edges, corners, probe, *dft_tables(),
    )


def gather_kernel(
    sums_ref,
    left_ref,
    right_ref,
    probe_sums_ref,
    probe_ref,
    row_out,
    side_out,
    corner_out,
    probe_out,
    across,
    along,
    partial,
    send_sem,
    recv_sem,
):
    blocks = sums_ref.shape[1] - PADDED_BLOCKS
    rows = sums_ref.shape[2] - 2 * RIM
    n_ty, n_tx = lax.axis_size("ty"), lax.axis_size("tx")
    ty, tx = lax.axis_index("ty"), lax.axis_index("tx")
    strip = M // n_tx
    mine = pl.ds(pl.multiple_of(tx * strip, strip), strip)

    def at(down, right):
        return lax.rem(ty + down, n_ty), lax.rem(tx + right, n_tx)

    peers = [at(0, j) for j in range(1, n_tx)] + [at(j, 0) for j in range(1, n_ty)]
    peers += [neighbour(down, right) for down, right in CORNERS]
    barrier = pltpu.get_barrier_semaphore()
    for peer in peers:
        pl.semaphore_signal(barrier, inc=1, device_id=peer, device_id_type=MESH_ID)
    pl.semaphore_wait(barrier, len(peers))

    started = [0]

    def send(source, target, peer):
        slot = started[0]
        started[0] += 1
        copy = pltpu.make_async_remote_copy(
            src_ref=source,
            dst_ref=target,
            send_sem=send_sem.at[slot],
            recv_sem=recv_sem.at[slot],
            device_id=peer,
            device_id_type=MESH_ID,
        )
        copy.start()
        return copy

    first = []
    for j in range(1, n_tx):
        peer = at(0, j)
        there = pl.ds(pl.multiple_of(peer[1] * strip, strip), strip)
        first.append(send(probe_sums_ref.at[:, there, :], across.at[j], peer))
    main = rows + rows // 2
    corner = RIM + RIM // 2
    inner = pl.ds(1, blocks)
    rims = [
        send(right_ref.at[pl.ds(0, main)], side_out.at[0], neighbour(0, 1)),
        send(left_ref.at[pl.ds(0, main)], side_out.at[1], neighbour(0, -1)),
        send(sums_ref.at[:, inner, pl.ds(RIM + rows, RIM), :], row_out.at[0], neighbour(1, 0)),
        send(sums_ref.at[:, inner, pl.ds(0, RIM), :], row_out.at[1], neighbour(-1, 0)),
    ]
    for number, (down, right) in enumerate(CORNERS):
        packed = left_ref if right == -1 else right_ref
        start = main + (0 if down == -1 else corner)
        rims.append(send(packed.at[pl.ds(start, corner)], corner_out.at[number], neighbour(down, right)))

    total = probe_sums_ref[:, mine, :]
    for j in range(1, n_tx):
        first[j - 1].wait_recv()
        total = total + across[j]
    partial[...] = total
    second = [send(partial, along.at[j], at(j, 0)) for j in range(1, n_ty)]
    for j in range(1, n_ty):
        second[j - 1].wait_recv()
        total = total + along[j]
    weight = total[2] + tiny_level
    for part in range(2):
        probe_out[part, mine, :] = probe_ref[part, mine, :] - total[part] / weight
    third = [send(probe_out.at[:, mine, :], probe_out.at[:, mine, :], at(0, j)) for j in range(1, n_tx)]
    for copy in first + second:
        copy.wait_send()
    for copy in third + rims:
        copy.wait()


def gather(sums, left, right, probe_sums, probe, n_ty, n_tx):
    blocks = sums.shape[1] - PADDED_BLOCKS
    rows = sums.shape[2] - 2 * RIM
    main = rows + rows // 2
    strip = M // n_tx
    copies = 2 * (n_tx - 1) + (n_ty - 1) + 4 + len(CORNERS)
    return pl.pallas_call(
        gather_kernel,
        out_shape=(
            jax.ShapeDtypeStruct((2, 3, blocks, RIM, LANES), F32),
            jax.ShapeDtypeStruct((2, main, LANES), F32),
            jax.ShapeDtypeStruct((len(CORNERS), RIM + RIM // 2, LANES), F32),
            jax.ShapeDtypeStruct((2, M, M), F32),
        ),
        in_specs=[anywhere()] * 3 + [in_vmem()] * 2,
        out_specs=(anywhere(),) * 3 + (in_vmem(),),
        scratch_shapes=[
            pltpu.VMEM((n_tx, 3, strip, M), F32),
            pltpu.VMEM((n_ty, 3, strip, M), F32),
            pltpu.VMEM((3, strip, M), F32),
            pltpu.SemaphoreType.DMA((copies,)),
            pltpu.SemaphoreType.DMA((copies,)),
        ],
        compiler_params=pltpu.CompilerParams(
            collective_id=1, has_side_effects=True, vmem_limit_bytes=16 << 20
        ),
        name="gather",
    )(sums, left, right, probe_sums, probe)


def update_kernel(object_ref, sums_ref, row_ref, side_ref, corner_ref, probe_ref, object_out, probe_out):
    blocks = sums_ref.shape[1] - PADDED_BLOCKS
    chunk = object_ref.shape[1]
    step, steps = pl.program_id(0), pl.num_programs(0)
    rows = chunk * steps_of(side_ref, chunk)
    half = rows // 2
    at = pl.multiple_of(step * chunk, chunk)
    low = lane_ids(chunk) < RIM
    first_step, last_step = step == 0, step == steps - 1

    @pl.when(first_step)
    def _():
        probe_out[...] = probe_ref[...]

    def rolled(value):
        return pltpu.roll(value, RIM, 1)

    for block in range(blocks):
        totals = []
        for kind in range(3):
            value = sums_ref[kind, 1 + block]
            above = first_step & is_inside(-1, 0)
            below = last_step & is_inside(1, 0)
            value = value + jnp.where(above, row_ref[0, kind, block], 0.0)
            value = value + jnp.where(below, row_ref[1, kind, block], 0.0)
            if block in (0, blocks - 1):
                side = 0 if block == 0 else 1
                right = -1 if block == 0 else 1
                lanes = low if block == 0 else ~low
                if kind < 2:
                    rim = side_ref[side, pl.ds(at, chunk), :]
                    rim = rolled(rim) if kind else rim
                else:
                    late = at >= half
                    start = pl.multiple_of(rows + at - jnp.where(late, half, 0), chunk)
                    rim = side_ref[side, pl.ds(start, chunk), :]
                    rim = jnp.where(late, rolled(rim), rim)
                value = value + jnp.where(lanes & is_inside(0, right), rim, 0.0)
                for vertical, here in ((-1, first_step), (1, last_step)):
                    number = CORNERS.index((-vertical, -right))
                    if kind < 2:
                        rim = corner_ref[number, :RIM, :]
                        rim = rolled(rim) if kind else rim
                    else:
                        rim = corner_ref[number, RIM:, :]
                        rim = jnp.concatenate([rim, rolled(rim)], axis=0)
                    value = value + jnp.where(lanes & (here & is_inside(vertical, right)), rim, 0.0)
            totals.append(value)
        lit = totals[2] + floor_level
        at_lanes = slice(block * LANES, (block + 1) * LANES)
        for part in range(2):
            object_out[part, :, at_lanes] = object_ref[part, :, at_lanes] - totals[part] / lit


def steps_of(side_ref, chunk):
    return side_ref.shape[1] * 2 // 3 // chunk


def update(object_field, sums, edges, sides, corners, probe):
    rows, cols = object_field.shape[1:]
    chunk = RIM
    whole = lambda array: pl.BlockSpec(array.shape, lambda i: (0,) * array.ndim, memory_space=pltpu.VMEM)
    return pl.pallas_call(
        update_kernel,
        grid=(rows // chunk,),
        out_shape=(
            jax.ShapeDtypeStruct(object_field.shape, F32),
            jax.ShapeDtypeStruct(probe.shape, F32),
        ),
        in_specs=[
            pl.BlockSpec((2, chunk, cols), lambda i: (0, i, 0)),
            pl.BlockSpec((3, sums.shape[1], chunk, LANES), lambda i: (0, 0, i + 1, 0)),
            whole(edges),
            whole(sides),
            whole(corners),
            whole(probe),
        ],
        out_specs=(pl.BlockSpec((2, chunk, cols), lambda i: (0, i, 0)), whole(probe)),
        compiler_params=pltpu.CompilerParams(vmem_limit_bytes=24 << 20),
        name="update",
    )(object_field, sums, edges, sides, corners, probe)


def solution(mesh):
    n_ty, n_tx = mesh.shape["ty"], mesh.shape["tx"]

    def shards(measured, positions, owners, counts, object_field, probe_field):
        own = measured[0, 0]
        arrived, tags, sides, edges, corners = spread(owners, positions, counts, own, object_field)
        sums, left, right, probe_sums = patterns(
            owners, positions, counts, tags, own, arrived, object_field, sides, edges, corners, probe_field
        )
        edge_sums, side_sums, corner_sums, new_probe = gather(
            sums, left, right, probe_sums, probe_field, n_ty, n_tx
        )
        return update(object_field, sums, edge_sums, side_sums, corner_sums, new_probe)

    placed = (
        P("ty", "tx", None, None, None),
        P("ty", "tx", None, None),
        P("ty", "tx", None),
        P("ty", "tx"),
        P(None, "ty", "tx"),
        P(),
    )
    return jax.shard_map(
        shards, mesh=mesh, in_specs=placed, out_specs=(P(None, "ty", "tx"), P()), check_vma=False
    )
```

```python
import functools

import jax
import jax.numpy as jnp
import numpy as np
from jax import lax
from jax.experimental import pallas as pl
from jax.experimental.pallas import tpu as pltpu
from jax.sharding import PartitionSpec as P

M = 128
MOVE = 2
RIM = M // 2
LANES = 128
PADDED_BLOCKS = 2
SPARE_BLOCKS = 2
BATCH = 4

offset_level = 1.0
floor_level = 1.0
tiny_level = 1e-06

MESH_ID = pl.DeviceIdType.MESH
DIRECTIONS = [(-1, -1), (-1, 0), (-1, 1), (0, -1), (0, 1), (1, -1), (1, 0), (1, 1)]
CORNERS = [(-1, -1), (-1, 1), (1, -1), (1, 1)]

F32 = jnp.float32
BF16 = jnp.bfloat16
I32 = jnp.int32


def in_vmem():
    return pl.BlockSpec(memory_space=pltpu.VMEM)


def in_smem():
    return pl.BlockSpec(memory_space=pltpu.SMEM)


def dft_tables():
    phase = (np.outer(np.arange(M), np.arange(M)) % M) * (2.0 * np.pi / M)
    c, s = np.cos(phase) / np.sqrt(M), -np.sin(phase) / np.sqrt(M)
    forward = np.block([[c, s], [-s, c]])
    tables = []
    for table in (forward, forward.T):
        high = table.astype(BF16)
        tables += [high, (table - high.astype(np.float64)).astype(BF16)]
    return np.stack(tables)


def lane_ids(rows):
    return lax.broadcasted_iota(I32, (rows, LANES), 1)


def neighbour(down, right):
    ty, tx = lax.axis_index("ty"), lax.axis_index("tx")
    n_ty, n_tx = lax.axis_size("ty"), lax.axis_size("tx")
    return lax.rem(ty + (down + n_ty), n_ty), lax.rem(tx + (right + n_tx), n_tx)


def is_inside(down, right):
    ty, tx = lax.axis_index("ty"), lax.axis_index("tx")
    row, col = ty + down, tx + right
    return (row >= 0) & (row < lax.axis_size("ty")) & (col >= 0) & (col < lax.axis_size("tx"))


def pack_left(first, second, rows):
    return jnp.where(lane_ids(rows) >= RIM, first, pltpu.roll(second, RIM, 1))


def pack_right(first, second, rows):
    return jnp.where(lane_ids(rows) < RIM, first, pltpu.roll(second, RIM, 1))


def in_hbm():
    return pl.BlockSpec(memory_space=pltpu.HBM)


def kept_in_hbm(array):
    return pltpu.with_memory_space_constraint(array, pltpu.HBM)


def spread_kernel(
    owners_ref,
    positions_ref,
    counts_ref,
    measured_ref,
    object_ref,
    probe_ref,
    tables_ref,
    field,
    data,
    tag_out,
    shifted,
    tables,
    sums,
    arrived,
    sides,
    corners,
    probe,
    pattern_pack,
    tag_pack,
    side_pack,
    local_sem,
    send_sem,
    recv_sem,
):
    slots = measured_ref.shape[0]
    rows, cols = object_ref.shape[1:]
    blocks = cols // LANES
    n_tx = lax.axis_size("tx")
    ty, tx = lax.axis_index("ty"), lax.axis_index("tx")

    barrier = pltpu.get_barrier_semaphore()
    for down, right in DIRECTIONS:
        pl.semaphore_signal(barrier, inc=1, device_id=neighbour(down, right), device_id_type=MESH_ID)

    local = []

    def fetch(source, target):
        copy = pltpu.make_async_copy(source, target, local_sem.at[len(local)])
        copy.start()
        local.append(copy)
        return copy

    inner_rows = pl.ds(RIM, rows)
    edge_blocks = [0, blocks - 1]
    own_blocks = []
    for group in (edge_blocks, range(1, blocks - 1)):
        for block in group:
            own_blocks.append(
                fetch(object_ref.at[:, :, pl.ds(block * LANES, LANES)], field.at[:, 1 + block, inner_rows, :])
            )
    own_data = fetch(measured_ref, data.at[pl.ds(0, slots)])
    own_probe = fetch(probe_ref, probe)
    own_tables = fetch(tables_ref, tables)

    for copy in own_blocks[:2]:
        copy.wait()
    last = (blocks, inner_rows, slice(None))
    side_pack[0] = pack_left(field[(0,) + last], field[(1,) + last], rows)
    side_pack[1] = pack_right(field[0, 1, inner_rows, :], field[1, 1, inner_rows, :], rows)
    pl.semaphore_wait(barrier, len(DIRECTIONS))

    started = [0]

    def send(source, target, down, right):
        slot = started[0]
        started[0] += 1
        copy = pltpu.make_async_remote_copy(
            src_ref=source,
            dst_ref=target,
            send_sem=send_sem.at[slot],
            recv_sem=recv_sem.at[slot],
            device_id=neighbour(down, right),
            device_id_type=MESH_ID,
        )
        copy.start()
        return copy

    rims = [send(side_pack.at[0], sides.at[0], 0, 1), send(side_pack.at[1], sides.at[1], 0, -1)]
    for corner, (down, right) in enumerate(CORNERS):
        source = side_pack.at[0 if right == 1 else 1, pl.ds(0 if down == -1 else rows - RIM, RIM), :]
        rims.append(send(source, corners.at[corner], down, right))
    for copy in own_blocks[2:]:
        copy.wait()
    inner = pl.ds(1, blocks)
    lines = [
        send(field.at[:, inner, pl.ds(rows, RIM), :], field.at[:, inner, pl.ds(0, RIM), :], 1, 0),
        send(field.at[:, inner, pl.ds(RIM, RIM), :], field.at[:, inner, pl.ds(RIM + rows, RIM), :], -1, 0),
    ]

    own_data.wait()
    count = counts_ref[0, 0]
    lane = lane_ids(1)
    moves = []
    for way, (down, right) in enumerate(DIRECTIONS):
        target = jnp.where(is_inside(down, right), (ty + down) * n_tx + (tx + right), -1)
        found, first, second = jnp.int32(0), jnp.int32(0), jnp.int32(0)
        for slot in range(slots):
            hit = (owners_ref[0, 0, slot] == target) & (slot < count)
            first = jnp.where(hit & (found == 0), slot, first)
            second = jnp.where(hit & (found == 1), slot, second)
            found = found + hit.astype(I32)
        tag = jnp.zeros((1, LANES), I32)
        for index, chosen in enumerate((first, second)):
            pattern_pack[way, index] = data[chosen]
            valid = (found > index).astype(I32)
            tag = jnp.where(lane == 3 * index, valid, tag)
            tag = jnp.where(lane == 3 * index + 1, positions_ref[0, chosen], tag)
            tag = jnp.where(lane == 3 * index + 2, positions_ref[1, chosen], tag)
        tag_pack[way] = tag
    for way, (down, right) in enumerate(DIRECTIONS):
        moves.append(send(tag_pack.at[way], tag_out.at[way], down, right))
        moves.append(send(pattern_pack.at[way], arrived.at[pl.ds(way * MOVE, MOVE)], down, right))

    sums[...] = jnp.zeros(sums.shape, F32)
    spare = pl.ds(blocks + PADDED_BLOCKS, SPARE_BLOCKS)
    field[:, spare, pl.ds(0, M + 8), :] = jnp.zeros((2, SPARE_BLOCKS, M + 8, LANES), F32)
    own_probe.wait()
    for turn in range(8):
        for part in range(2):
            value = probe[part]
            shifted[turn, part] = pltpu.roll(value, turn, 0) if turn else value

    def unpacked(part, value):
        return value if part == 0 else pltpu.roll(value, RIM, 1)

    for copy in rims[:2]:
        copy.wait_recv()
    for part in range(2):
        field[part, 0, inner_rows, :] = jnp.where(is_inside(0, -1), unpacked(part, sides[0]), 0.0)
        field[part, 1 + blocks, inner_rows, :] = jnp.where(is_inside(0, 1), unpacked(part, sides[1]), 0.0)
    for corner, (down, right) in enumerate(CORNERS):
        rims[2 + corner].wait_recv()
        here = pl.ds(0, RIM) if down == 1 else pl.ds(RIM + rows, RIM)
        for part in range(2):
            field[part, 0 if right == 1 else 1 + blocks, here, :] = jnp.where(
                is_inside(-down, -right), unpacked(part, corners[corner]), 0.0
            )
    for line, (down, here) in zip(lines, ((-1, pl.ds(0, RIM)), (1, pl.ds(RIM + rows, RIM)))):
        line.wait()

        @pl.when(jnp.logical_not(is_inside(down, 0)))
        def _():
            field[:, inner, here, :] = jnp.zeros((2, blocks, RIM, LANES), F32)

    for copy in moves:
        copy.wait_recv()
    data[pl.ds(slots, arrived.shape[0])] = arrived[...]
    for copy in rims + moves:
        copy.wait_send()
    own_tables.wait()


def spread(owners, positions, counts, measured, object_field, probe_field):
    slots = measured.shape[0]
    rows, cols = object_field.shape[1:]
    blocks = cols // LANES
    ways = len(DIRECTIONS)
    copies = 4 + len(CORNERS) + 2 * ways
    all_blocks = blocks + PADDED_BLOCKS + SPARE_BLOCKS
    return pl.pallas_call(
        spread_kernel,
        out_shape=(
            jax.ShapeDtypeStruct((2, all_blocks, rows + 2 * RIM, LANES), F32),
            jax.ShapeDtypeStruct((slots + ways * MOVE, M, M), F32),
            jax.ShapeDtypeStruct((ways, 1, LANES), I32),
            jax.ShapeDtypeStruct((8, 2, M, M), F32),
            jax.ShapeDtypeStruct((4, 2 * M, 2 * M), BF16),
            jax.ShapeDtypeStruct((3, all_blocks, rows + 2 * RIM, LANES), F32),
        ),
        in_specs=[in_smem()] * 3 + [in_hbm()] * 4,
        out_specs=(in_vmem(),) * 6,
        scratch_shapes=[
            pltpu.VMEM((ways * MOVE, M, M), F32),
            pltpu.VMEM((2, rows, LANES), F32),
            pltpu.VMEM((len(CORNERS), RIM, LANES), F32),
            pltpu.VMEM((2, M, M), F32),
            pltpu.VMEM((ways, MOVE, M, M), F32),
            pltpu.VMEM((ways, 1, LANES), I32),
            pltpu.VMEM((2, rows, LANES), F32),
            pltpu.SemaphoreType.DMA((blocks + 3,)),
            pltpu.SemaphoreType.DMA((copies,)),
            pltpu.SemaphoreType.DMA((copies,)),
        ],
        compiler_params=pltpu.CompilerParams(
            collective_id=0, has_side_effects=True, vmem_limit_bytes=12 << 20
        ),
        name="spread",
    )(owners, positions, counts, *(kept_in_hbm(x) for x in (measured, object_field, probe_field, dft_tables())))


def dot(a, b):
    return jnp.dot(a, b, preferred_element_type=F32)


def patterns_kernel(
    owners_ref,
    positions_ref,
    counts_ref,
    tag_ref,
    data,
    field,
    shifted,
    tables,
    _,
    sums_ref,
    left_ref,
    right_ref,
    probe_sums_ref,
    turned_sums,
    window,
    framed,
    operands,
    row_list,
    col_list,
    data_list,
):
    slots = owners_ref.shape[2]
    rows = sums_ref.shape[2] - 2 * RIM
    blocks = sums_ref.shape[1] - PADDED_BLOCKS - SPARE_BLOCKS
    n_tx = lax.axis_size("tx")
    ty, tx = lax.axis_index("ty"), lax.axis_index("tx")
    self_index = ty * n_tx + tx
    forward, backward = (tables.at[0], tables.at[1]), (tables.at[2], tables.at[3])

    turned_sums[...] = jnp.zeros(turned_sums.shape, F32)

    count = counts_ref[0, 0]

    def own(slot, total):
        row_list[total] = positions_ref[0, slot]
        col_list[total] = positions_ref[1, slot]
        data_list[total] = slot
        return total + ((owners_ref[0, 0, slot] == self_index) & (slot < count)).astype(I32)

    total = lax.fori_loop(0, slots, own, jnp.int32(0), unroll=4)
    for way in range(len(DIRECTIONS)):
        for index in range(MOVE):
            row_list[total] = tag_ref[way, 0, 3 * index + 1]
            col_list[total] = tag_ref[way, 0, 3 * index + 2]
            data_list[total] = slots + way * MOVE + index
            total = total + tag_ref[way, 0, 3 * index]
    for index in range(BATCH):
        row_list[total + index] = 0
        col_list[total + index] = (blocks + PADDED_BLOCKS) * LANES - RIM
        data_list[total + index] = 0

    lane_of_frame = lane_ids(M)
    lane_of_window = lane_ids(M + 8)
    row_of_tile = lax.broadcasted_iota(I32, (8, LANES), 0)

    def place(step, index):
        number = step * BATCH + index
        row, col = row_list[number], col_list[number] + RIM
        turn, lane = row & 7, col & (LANES - 1)
        return number, pl.multiple_of(row - turn, 8), lax.shift_right_logical(col, 7), turn, lane

    def put_split(stage, pair, at, value):
        operands[stage, 0, pair, at[0], at[1]] = value.astype(BF16)
        low = value - operands[stage, 0, pair, at[0], at[1]].astype(F32)
        operands[stage, 1, pair, at[0], at[1]] = low.astype(BF16)

    def square(row, col):
        return pl.ds(row * M, M), pl.ds(col * M, M)

    def load(step, pair):
        for half in range(2):
            index = 2 * pair + half
            _, row, block, turn, lane = place(step, index)
            later = lane_of_window >= lane
            kept = row_of_tile >= turn
            parts = []
            for part in range(2):
                here = field[part, block, pl.ds(row, M + 8), :]
                beside = field[part, block + 1, pl.ds(row, M + 8), :]
                value = jnp.where(later, here, beside)
                value = jnp.concatenate([jnp.where(kept, value[:8], value[M:]), value[8:M]], axis=0)
                window[index, part] = value
                parts.append(value)
            wr, wi = parts
            pr = pltpu.roll(shifted[turn, 0], lane, 1)
            pi = pltpu.roll(shifted[turn, 1], lane, 1)
            framed[index, 0] = pr
            framed[index, 1] = pi
            put_split(0, pair, square(half, 0), pr * wr - pi * wi)
            put_split(0, pair, square(half, 1), pr * wi + pi * wr)

    def right_product(stage, pair, table):
        high, low = table
        a, b = operands[stage, 0, pair], operands[stage, 1, pair]
        value = dot(a, high[...]) + dot(b, high[...]) + dot(a, low[...])
        for half in range(2):
            for part in range(2):
                piece = value[half * M : (half + 1) * M, part * M : (part + 1) * M]
                put_split(stage + 1, pair, square(part, half), piece)

    def left_product(stage, pair, table):
        high, low = table
        a, b = operands[stage, 0, pair], operands[stage, 1, pair]
        return dot(high[...], a) + dot(high[...], b) + dot(low[...], a)

    def first_right(step, pair):
        right_product(0, pair, forward)

    def first_left(step, pair):
        far = left_product(1, pair, backward)
        for half in range(2):
            fr = far[:M, half * M : (half + 1) * M]
            fi = far[M:, half * M : (half + 1) * M]
            measured = data[data_list[step * BATCH + 2 * pair + half]]
            ratio = 1.0 - measured / (fr * fr + fi * fi + offset_level)
            put_split(2, pair, square(half, 0), fr * ratio)
            put_split(2, pair, square(half, 1), fi * ratio)

    def second_right(step, pair):
        right_product(2, pair, backward)

    def second_left(step, pair):
        back = left_product(3, pair, forward)
        for half in range(2):
            index = 2 * pair + half
            _, row, block, turn, lane = place(step, index)
            cr = back[:M, half * M : (half + 1) * M]
            ci = back[M:, half * M : (half + 1) * M]
            wr, wi = window[index, 0], window[index, 1]
            pr, pi = framed[index, 0], framed[index, 1]
            back_lanes = (LANES - lane) & (LANES - 1)
            terms = (wr * cr + wi * ci, wr * ci - wi * cr, wr * wr + wi * wi)
            for kind, term in enumerate(terms):
                turned_sums[turn, kind] += pltpu.roll(term, back_lanes, 1)
            later = lane_of_frame >= lane
            kept = row_of_tile >= turn
            terms = (pr * cr + pi * ci, pr * ci - pi * cr, pr * pr + pi * pi)
            for kind, term in enumerate(terms):
                for beside in range(2):
                    piece = jnp.where(later, 0.0, term) if beside else jnp.where(later, term, 0.0)
                    top = piece[:8]
                    piece = jnp.concatenate(
                        [jnp.where(kept, top, 0.0), piece[8:], jnp.where(kept, 0.0, top)], axis=0
                    )
                    sums_ref[kind, block + beside, pl.ds(row, M + 8), :] += piece

    phases = (load, first_right, first_left, second_right, second_left)
    pairs = BATCH // 2

    def one_batch(step, carry):
        for turn in range(len(phases) + pairs - 1):
            for pair in range(pairs):
                if 0 <= turn - pair < len(phases):
                    phases[turn - pair](step, pair)
        return carry

    lax.fori_loop(0, lax.div(total + (BATCH - 1), BATCH), one_batch, 0)

    for kind in range(3):
        total_of_kind = turned_sums[0, kind]
        for turn in range(1, 8):
            total_of_kind = total_of_kind + pltpu.roll(turned_sums[turn, kind], M - turn, 0)
        probe_sums_ref[kind] = total_of_kind

    half = rows // 2
    for pack, out, block in ((pack_left, left_ref, 0), (pack_right, right_ref, 1 + blocks)):
        def rim(kind, start, length):
            return sums_ref[kind, block, start : start + length, :]

        out[:rows, :] = pack(rim(0, RIM, rows), rim(1, RIM, rows), rows)
        out[rows : rows + half, :] = pack(rim(2, RIM, half), rim(2, RIM + half, half), half)
        at = rows + half
        for start in (0, RIM + rows):
            out[at : at + RIM, :] = pack(rim(0, start, RIM), rim(1, start, RIM), RIM)
            out[at + RIM : at + RIM + RIM // 2, :] = pack(
                rim(2, start, RIM // 2), rim(2, start + RIM // 2, RIM // 2), RIM // 2
            )
            at += RIM + RIM // 2


def patterns(owners, positions, counts, tags, data, field, shifted, tables, sums):
    rows = sums.shape[2] - 2 * RIM
    packed = rows + rows // 2 + 3 * RIM
    entries = data.shape[0] + BATCH
    return pl.pallas_call(
        patterns_kernel,
        out_shape=(
            jax.ShapeDtypeStruct(sums.shape, F32),
            jax.ShapeDtypeStruct((packed, LANES), F32),
            jax.ShapeDtypeStruct((packed, LANES), F32),
            jax.ShapeDtypeStruct((3, M, M), F32),
        ),
        in_specs=[in_smem()] * 4 + [in_vmem()] * 5,
        out_specs=(in_vmem(),) * 4,
        scratch_shapes=[
            pltpu.VMEM((8, 3, M, M), F32),
            pltpu.VMEM((BATCH, 2, M, M), F32),
            pltpu.VMEM((BATCH, 2, M, M), F32),
            pltpu.VMEM((4, 2, BATCH // 2, 2 * M, 2 * M), BF16),
            pltpu.SMEM((entries,), I32),
            pltpu.SMEM((entries,), I32),
            pltpu.SMEM((entries,), I32),
        ],
        input_output_aliases={8: 0},
        compiler_params=pltpu.CompilerParams(vmem_limit_bytes=16 << 20),
        name="patterns",
    )(owners, positions, counts, tags, data, field, shifted, tables, sums)


def gather_kernel(
    sums_ref,
    left_ref,
    right_ref,
    probe_sums_ref,
    probe_ref,
    field_ref,
    object_out,
    probe_out,
    lines,
    sides,
    corners,
    across,
    along,
    partial,
    send_sem,
    recv_sem,
):
    blocks = sums_ref.shape[1] - PADDED_BLOCKS - SPARE_BLOCKS
    rows = sums_ref.shape[2] - 2 * RIM
    half = rows // 2
    n_ty, n_tx = lax.axis_size("ty"), lax.axis_size("tx")
    ty, tx = lax.axis_index("ty"), lax.axis_index("tx")
    strip = M // n_tx
    mine = pl.ds(pl.multiple_of(tx * strip, strip), strip)

    def at(down, right):
        return lax.rem(ty + down, n_ty), lax.rem(tx + right, n_tx)

    peers = [at(0, j) for j in range(1, n_tx)] + [at(j, 0) for j in range(1, n_ty)]
    peers += [neighbour(down, right) for down, right in CORNERS]
    barrier = pltpu.get_barrier_semaphore()
    for peer in peers:
        pl.semaphore_signal(barrier, inc=1, device_id=peer, device_id_type=MESH_ID)
    pl.semaphore_wait(barrier, len(peers))

    started = [0]

    def send(source, target, peer):
        slot = started[0]
        started[0] += 1
        copy = pltpu.make_async_remote_copy(
            src_ref=source,
            dst_ref=target,
            send_sem=send_sem.at[slot],
            recv_sem=recv_sem.at[slot],
            device_id=peer,
            device_id_type=MESH_ID,
        )
        copy.start()
        return copy

    first = []
    for j in range(1, n_tx):
        peer = at(0, j)
        there = pl.ds(pl.multiple_of(peer[1] * strip, strip), strip)
        first.append(send(probe_sums_ref.at[:, there, :], across.at[j], peer))
    main = rows + half
    corner = RIM + RIM // 2
    inner = pl.ds(1, blocks)
    rims = [
        send(right_ref.at[pl.ds(0, main)], sides.at[0], neighbour(0, 1)),
        send(left_ref.at[pl.ds(0, main)], sides.at[1], neighbour(0, -1)),
        send(sums_ref.at[:, inner, pl.ds(RIM + rows, RIM), :], lines.at[0], neighbour(1, 0)),
        send(sums_ref.at[:, inner, pl.ds(0, RIM), :], lines.at[1], neighbour(-1, 0)),
    ]
    for number, (down, right) in enumerate(CORNERS):
        packed = left_ref if right == -1 else right_ref
        start = main + (0 if down == -1 else corner)
        rims.append(send(packed.at[pl.ds(start, corner)], corners.at[number], neighbour(down, right)))

    def rolled(value):
        return pltpu.roll(value, RIM, 1)

    def finish(block, start, length, totals):
        here = pl.ds(start, length)
        lit = 1.0 / (totals[2] + floor_level)
        for part in range(2):
            old = field_ref[part, 1 + block, pl.ds(start + RIM, length), :]
            object_out[part, here, block * LANES : (block + 1) * LANES] = old - totals[part] * lit

    def own(block, start, length):
        return [sums_ref[kind, 1 + block, pl.ds(start + RIM, length), :] for kind in range(3)]

    def side(block, start, length, late):
        index, right = (0, -1) if block == 0 else (1, 1)
        low = lane_ids(length) < RIM
        lanes = (low if block == 0 else jnp.logical_not(low)) & is_inside(0, right)
        there = sides[index, pl.ds(start, length), :]
        light = sides[index, pl.ds(start + (rows - half if late else rows), length), :]
        values = (there, rolled(there), rolled(light) if late else light)
        return [jnp.where(lanes, value, 0.0) for value in values]

    def plus(a, b):
        return [x + y for x, y in zip(a, b)]

    chunk = RIM

    def middle(step, carry):
        start = pl.multiple_of(step * chunk, chunk)
        for block in range(1, blocks - 1):
            finish(block, start, chunk, own(block, start, chunk))
        return carry

    lax.fori_loop(1, rows // chunk - 1, middle, 0)

    total = probe_sums_ref[:, mine, :]
    for j in range(1, n_tx):
        first[j - 1].wait_recv()
        total = total + across[j]
    partial[...] = total
    second = [send(partial, along.at[j], at(j, 0)) for j in range(1, n_ty)]
    for j in range(1, n_ty):
        second[j - 1].wait_recv()
        total = total + along[j]
    weight = total[2] + tiny_level
    for part in range(2):
        probe_out[part, mine, :] = probe_ref[part, mine, :] - total[part] / weight
    third = [send(probe_out.at[:, mine, :], probe_out.at[:, mine, :], at(0, j)) for j in range(1, n_tx)]

    for copy in rims:
        copy.wait_recv()
    for late in (False, True):

        def outer(step, carry):
            start = pl.multiple_of(step * chunk, chunk)
            for block in (0, blocks - 1):
                finish(block, start, chunk, plus(own(block, start, chunk), side(block, start, chunk, late)))
            return carry

        middle_step = half // chunk
        lax.fori_loop(*((middle_step, rows // chunk - 1) if late else (1, middle_step)), outer, 0)
    for line, down in enumerate((-1, 1)):
        start = 0 if down == -1 else rows - RIM
        for block in range(blocks):
            totals = own(block, start, RIM)
            arrived = [jnp.where(is_inside(down, 0), lines[line, kind, block], 0.0) for kind in range(3)]
            totals = plus(totals, arrived)
            if block in (0, blocks - 1):
                totals = plus(totals, side(block, start, RIM, down == 1))
                right = -1 if block == 0 else 1
                number = CORNERS.index((-down, -right))
                low = lane_ids(RIM) < RIM
                lanes = (low if block == 0 else jnp.logical_not(low)) & is_inside(down, right)
                there = corners[number, :RIM, :]
                light = corners[number, RIM:, :]
                values = (there, rolled(there), jnp.concatenate([light, rolled(light)], axis=0))
                totals = plus(totals, [jnp.where(lanes, value, 0.0) for value in values])
            finish(block, start, RIM, totals)

    for copy in first + second + rims:
        copy.wait_send()
    for copy in third:
        copy.wait()


def gather(sums, left, right, probe_sums, probe, field, n_ty, n_tx):
    blocks = sums.shape[1] - PADDED_BLOCKS - SPARE_BLOCKS
    rows = sums.shape[2] - 2 * RIM
    main = rows + rows // 2
    strip = M // n_tx
    copies = 2 * (n_tx - 1) + (n_ty - 1) + 4 + len(CORNERS)
    return pl.pallas_call(
        gather_kernel,
        out_shape=(
            jax.ShapeDtypeStruct((2, rows, blocks * LANES), F32),
            jax.ShapeDtypeStruct((2, M, M), F32),
        ),
        in_specs=[in_vmem()] * 6,
        out_specs=(in_vmem(),) * 2,
        scratch_shapes=[
            pltpu.VMEM((2, 3, blocks, RIM, LANES), F32),
            pltpu.VMEM((2, main, LANES), F32),
            pltpu.VMEM((len(CORNERS), RIM + RIM // 2, LANES), F32),
            pltpu.VMEM((n_tx, 3, strip, M), F32),
            pltpu.VMEM((n_ty, 3, strip, M), F32),
            pltpu.VMEM((3, strip, M), F32),
            pltpu.SemaphoreType.DMA((copies,)),
            pltpu.SemaphoreType.DMA((copies,)),
        ],
        compiler_params=pltpu.CompilerParams(
            collective_id=1, has_side_effects=True, vmem_limit_bytes=12 << 20
        ),
        name="gather",
    )(sums, left, right, probe_sums, probe, field)


def solution(mesh):
    n_ty, n_tx = mesh.shape["ty"], mesh.shape["tx"]

    def shards(measured, positions, owners, counts, object_field, probe_field):
        positions, owners = kept_in_hbm(positions[0, 0].T), kept_in_hbm(owners)
        field, data, tags, shifted, tables, sums = spread(
            owners, positions, counts, measured[0, 0], object_field, probe_field
        )
        sums, left, right, probe_sums = patterns(
            owners, positions, counts, tags, data, field, shifted, tables, sums
        )
        return gather(sums, left, right, probe_sums, probe_field, field, n_ty, n_tx)

    placed = (
        P("ty", "tx", None, None, None),
        P("ty", "tx", None, None),
        P("ty", "tx", None),
        P("ty", "tx"),
        P(None, "ty", "tx"),
        P(),
    )
    return jax.shard_map(
        shards, mesh=mesh, in_specs=placed, out_specs=(P(None, "ty", "tx"), P()), check_vma=False
    )
```

```python
import functools

import jax
import jax.numpy as jnp
import numpy as np
from jax import lax
from jax.experimental import pallas as pl
from jax.experimental.pallas import tpu as pltpu
from jax.sharding import PartitionSpec as P

M = 128
MOVE = 2
RIM = M // 2
LANES = 128
PADDED_BLOCKS = 2
SPARE_BLOCKS = 2
CHUNK = 16
BATCH = 4

offset_level = 1.0
floor_level = 1.0
tiny_level = 1e-06

MESH_ID = pl.DeviceIdType.MESH
DIRECTIONS = [(-1, -1), (-1, 0), (-1, 1), (0, -1), (0, 1), (1, -1), (1, 0), (1, 1)]
CORNERS = [(-1, -1), (-1, 1), (1, -1), (1, 1)]

F32 = jnp.float32
BF16 = jnp.bfloat16
I32 = jnp.int32


def in_vmem():
    return pl.BlockSpec(memory_space=pltpu.VMEM)


def in_smem():
    return pl.BlockSpec(memory_space=pltpu.SMEM)


def dft_tables():
    phase = (np.outer(np.arange(M), np.arange(M)) % M) * (2.0 * np.pi / M)
    c, s = np.cos(phase) / np.sqrt(M), -np.sin(phase) / np.sqrt(M)
    forward = np.block([[c, s], [-s, c]])
    tables = []
    for table in (forward, forward.T):
        high = table.astype(BF16)
        tables += [high, (table - high.astype(np.float64)).astype(BF16)]
    return np.stack(tables)


def lane_ids(rows):
    return lax.broadcasted_iota(I32, (rows, LANES), 1)


def neighbour(down, right):
    ty, tx = lax.axis_index("ty"), lax.axis_index("tx")
    n_ty, n_tx = lax.axis_size("ty"), lax.axis_size("tx")
    return lax.rem(ty + (down + n_ty), n_ty), lax.rem(tx + (right + n_tx), n_tx)


def is_inside(down, right):
    ty, tx = lax.axis_index("ty"), lax.axis_index("tx")
    row, col = ty + down, tx + right
    return (row >= 0) & (row < lax.axis_size("ty")) & (col >= 0) & (col < lax.axis_size("tx"))


def pack_left(first, second, rows):
    return jnp.where(lane_ids(rows) >= RIM, first, pltpu.roll(second, RIM, 1))


def pack_right(first, second, rows):
    return jnp.where(lane_ids(rows) < RIM, first, pltpu.roll(second, RIM, 1))


def in_hbm():
    return pl.BlockSpec(memory_space=pltpu.HBM)


def kept_in_hbm(array):
    return pltpu.with_memory_space_constraint(array, pltpu.HBM)


def spread_kernel(
    owners_ref,
    positions_ref,
    counts_ref,
    measured_ref,
    object_ref,
    probe_ref,
    tables_ref,
    field,
    data,
    tag_out,
    shifted,
    tables,
    sums,
    arrived,
    sides,
    corners,
    probe,
    pattern_pack,
    tag_pack,
    side_pack,
    local_sem,
    send_sem,
    recv_sem,
):
    slots = measured_ref.shape[0]
    rows, cols = object_ref.shape[1:]
    blocks = cols // LANES
    n_tx = lax.axis_size("tx")
    ty, tx = lax.axis_index("ty"), lax.axis_index("tx")

    barrier = pltpu.get_barrier_semaphore()
    for down, right in DIRECTIONS:
        pl.semaphore_signal(barrier, inc=1, device_id=neighbour(down, right), device_id_type=MESH_ID)

    local = []

    def fetch(source, target):
        copy = pltpu.make_async_copy(source, target, local_sem.at[len(local)])
        copy.start()
        local.append(copy)
        return copy

    inner_rows = pl.ds(RIM, rows)
    edge_blocks = [0, blocks - 1]
    own_blocks = []
    for group in (edge_blocks, range(1, blocks - 1)):
        for block in group:
            own_blocks.append(
                fetch(object_ref.at[:, :, pl.ds(block * LANES, LANES)], field.at[:, 1 + block, inner_rows, :])
            )
    own_data = fetch(measured_ref, data.at[pl.ds(0, slots)])
    own_probe = fetch(probe_ref, probe)
    own_tables = fetch(tables_ref, tables)

    for copy in own_blocks[:2]:
        copy.wait()
    last = (blocks, inner_rows, slice(None))
    side_pack[0] = pack_left(field[(0,) + last], field[(1,) + last], rows)
    side_pack[1] = pack_right(field[0, 1, inner_rows, :], field[1, 1, inner_rows, :], rows)
    pl.semaphore_wait(barrier, len(DIRECTIONS))

    started = [0]

    def send(source, target, down, right):
        slot = started[0]
        started[0] += 1
        copy = pltpu.make_async_remote_copy(
            src_ref=source,
            dst_ref=target,
            send_sem=send_sem.at[slot],
            recv_sem=recv_sem.at[slot],
            device_id=neighbour(down, right),
            device_id_type=MESH_ID,
        )
        copy.start()
        return copy

    rims = [send(side_pack.at[0], sides.at[0], 0, 1), send(side_pack.at[1], sides.at[1], 0, -1)]
    for corner, (down, right) in enumerate(CORNERS):
        source = side_pack.at[0 if right == 1 else 1, pl.ds(0 if down == -1 else rows - RIM, RIM), :]
        rims.append(send(source, corners.at[corner], down, right))
    for copy in own_blocks[2:]:
        copy.wait()
    inner = pl.ds(1, blocks)
    lines = [
        send(field.at[:, inner, pl.ds(rows, RIM), :], field.at[:, inner, pl.ds(0, RIM), :], 1, 0),
        send(field.at[:, inner, pl.ds(RIM, RIM), :], field.at[:, inner, pl.ds(RIM + rows, RIM), :], -1, 0),
    ]

    own_data.wait()
    count = counts_ref[0, 0]
    lane = lane_ids(1)
    moves = []
    for way, (down, right) in enumerate(DIRECTIONS):
        target = jnp.where(is_inside(down, right), (ty + down) * n_tx + (tx + right), -1)
        found, first, second = jnp.int32(0), jnp.int32(0), jnp.int32(0)
        for slot in range(slots):
            hit = (owners_ref[0, 0, slot] == target) & (slot < count)
            first = jnp.where(hit & (found == 0), slot, first)
            second = jnp.where(hit & (found == 1), slot, second)
            found = found + hit.astype(I32)
        tag = jnp.zeros((1, LANES), I32)
        for index, chosen in enumerate((first, second)):
            pattern_pack[way, index] = data[chosen]
            valid = (found > index).astype(I32)
            tag = jnp.where(lane == 3 * index, valid, tag)
            tag = jnp.where(lane == 3 * index + 1, positions_ref[0, chosen], tag)
            tag = jnp.where(lane == 3 * index + 2, positions_ref[1, chosen], tag)
        tag_pack[way] = tag
    for way, (down, right) in enumerate(DIRECTIONS):
        moves.append(send(tag_pack.at[way], tag_out.at[way], down, right))
        moves.append(send(pattern_pack.at[way], arrived.at[pl.ds(way * MOVE, MOVE)], down, right))

    sums[...] = jnp.zeros(sums.shape, F32)
    spare = pl.ds(blocks + PADDED_BLOCKS, SPARE_BLOCKS)
    field[:, spare, pl.ds(0, M + 8), :] = jnp.zeros((2, SPARE_BLOCKS, M + 8, LANES), F32)
    own_probe.wait()
    for turn in range(8):
        for part in range(2):
            value = probe[part]
            shifted[turn, part] = pltpu.roll(value, turn, 0) if turn else value

    def unpacked(part, value):
        return value if part == 0 else pltpu.roll(value, RIM, 1)

    for copy in rims[:2]:
        copy.wait_recv()
    for part in range(2):
        field[part, 0, inner_rows, :] = jnp.where(is_inside(0, -1), unpacked(part, sides[0]), 0.0)
        field[part, 1 + blocks, inner_rows, :] = jnp.where(is_inside(0, 1), unpacked(part, sides[1]), 0.0)
    for corner, (down, right) in enumerate(CORNERS):
        rims[2 + corner].wait_recv()
        here = pl.ds(0, RIM) if down == 1 else pl.ds(RIM + rows, RIM)
        for part in range(2):
            field[part, 0 if right == 1 else 1 + blocks, here, :] = jnp.where(
                is_inside(-down, -right), unpacked(part, corners[corner]), 0.0
            )
    for line, (down, here) in zip(lines, ((-1, pl.ds(0, RIM)), (1, pl.ds(RIM + rows, RIM)))):
        line.wait()

        @pl.when(jnp.logical_not(is_inside(down, 0)))
        def _():
            field[:, inner, here, :] = jnp.zeros((2, blocks, RIM, LANES), F32)

    for copy in moves:
        copy.wait_recv()
    data[pl.ds(slots, arrived.shape[0])] = arrived[...]
    for copy in rims + moves:
        copy.wait_send()
    own_tables.wait()


def spread(owners, positions, counts, measured, object_field, probe_field):
    slots = measured.shape[0]
    rows, cols = object_field.shape[1:]
    blocks = cols // LANES
    ways = len(DIRECTIONS)
    copies = 4 + len(CORNERS) + 2 * ways
    all_blocks = blocks + PADDED_BLOCKS + SPARE_BLOCKS
    return pl.pallas_call(
        spread_kernel,
        out_shape=(
            jax.ShapeDtypeStruct((2, all_blocks, rows + 2 * RIM, LANES), F32),
            jax.ShapeDtypeStruct((slots + ways * MOVE, M, M), F32),
            jax.ShapeDtypeStruct((ways, 1, LANES), I32),
            jax.ShapeDtypeStruct((8, 2, M, M), F32),
            jax.ShapeDtypeStruct((4, 2 * M, 2 * M), BF16),
            jax.ShapeDtypeStruct((3, all_blocks, rows + 2 * RIM, LANES), F32),
        ),
        in_specs=[in_smem()] * 3 + [in_hbm()] * 4,
        out_specs=(in_vmem(),) * 6,
        scratch_shapes=[
            pltpu.VMEM((ways * MOVE, M, M), F32),
            pltpu.VMEM((2, rows, LANES), F32),
            pltpu.VMEM((len(CORNERS), RIM, LANES), F32),
            pltpu.VMEM((2, M, M), F32),
            pltpu.VMEM((ways, MOVE, M, M), F32),
            pltpu.VMEM((ways, 1, LANES), I32),
            pltpu.VMEM((2, rows, LANES), F32),
            pltpu.SemaphoreType.DMA((blocks + 3,)),
            pltpu.SemaphoreType.DMA((copies,)),
            pltpu.SemaphoreType.DMA((copies,)),
        ],
        compiler_params=pltpu.CompilerParams(
            collective_id=0, has_side_effects=True, vmem_limit_bytes=12 << 20
        ),
        name="spread",
    )(owners, positions, counts, *(kept_in_hbm(x) for x in (measured, object_field, probe_field, dft_tables())))


def dot(a, b):
    return jnp.dot(a, b, preferred_element_type=F32)


def patterns_kernel(
    owners_ref,
    positions_ref,
    counts_ref,
    tag_ref,
    data,
    field,
    shifted,
    tables,
    _,
    sums_ref,
    left_ref,
    right_ref,
    probe_sums_ref,
    turned_sums,
    window,
    framed,
    operands,
    row_list,
    col_list,
    data_list,
):
    slots = owners_ref.shape[2]
    rows = sums_ref.shape[2] - 2 * RIM
    blocks = sums_ref.shape[1] - PADDED_BLOCKS - SPARE_BLOCKS
    n_tx = lax.axis_size("tx")
    ty, tx = lax.axis_index("ty"), lax.axis_index("tx")
    self_index = ty * n_tx + tx
    forward, backward = (tables.at[0], tables.at[1]), (tables.at[2], tables.at[3])

    turned_sums[...] = jnp.zeros(turned_sums.shape, F32)

    count = counts_ref[0, 0]

    def own(slot, total):
        row_list[total] = positions_ref[0, slot]
        col_list[total] = positions_ref[1, slot]
        data_list[total] = slot
        return total + ((owners_ref[0, 0, slot] == self_index) & (slot < count)).astype(I32)

    total = lax.fori_loop(0, slots, own, jnp.int32(0), unroll=4)
    for way in range(len(DIRECTIONS)):
        for index in range(MOVE):
            row_list[total] = tag_ref[way, 0, 3 * index + 1]
            col_list[total] = tag_ref[way, 0, 3 * index + 2]
            data_list[total] = slots + way * MOVE + index
            total = total + tag_ref[way, 0, 3 * index]
    for index in range(BATCH):
        row_list[total + index] = 0
        col_list[total + index] = (blocks + PADDED_BLOCKS) * LANES - RIM
        data_list[total + index] = 0

    lane_of_chunk = lane_ids(CHUNK)
    row_of_tile = lax.broadcasted_iota(I32, (8, LANES), 0)

    def place(step, index):
        number = step * BATCH + index
        row, col = row_list[number], col_list[number] + RIM
        turn, lane = row & 7, col & (LANES - 1)
        return number, pl.multiple_of(row - turn, 8), lax.shift_right_logical(col, 7), turn, lane

    def put_split(stage, pair, at, value):
        operands[stage, 0, pair, at[0], at[1]] = value.astype(BF16)
        low = value - operands[stage, 0, pair, at[0], at[1]].astype(F32)
        operands[stage, 1, pair, at[0], at[1]] = low.astype(BF16)

    def strip(row, col, start):
        return pl.ds(row * M + start, CHUNK), pl.ds(col * M, M)

    def load(step, pair):
        for half in range(2):
            index = 2 * pair + half
            _, row, block, turn, lane = place(step, index)
            later = lane_of_chunk >= lane
            kept = row_of_tile >= turn
            kept_at = lax.rem(step, 2) * BATCH + index
            for start in range(0, M, CHUNK):
                rows_now = pl.ds(start, CHUNK)
                parts = []
                for part in range(2):
                    there = pl.ds(pl.multiple_of(row + start, 8), CHUNK)
                    value = jnp.where(later, field[part, block, there, :], field[part, block + 1, there, :])
                    if start == 0:
                        there = pl.ds(pl.multiple_of(row + M, 8), 8)
                        after = jnp.where(later[:8], field[part, block, there, :], field[part, block + 1, there, :])
                        value = jnp.concatenate([jnp.where(kept, value[:8], after), value[8:]], axis=0)
                    window[kept_at, part, rows_now, :] = value
                    parts.append(value)
                wr, wi = parts
                pr = pltpu.roll(shifted[turn, 0, rows_now, :], lane, 1)
                pi = pltpu.roll(shifted[turn, 1, rows_now, :], lane, 1)
                framed[kept_at, 0, rows_now, :] = pr
                framed[kept_at, 1, rows_now, :] = pi
                put_split(0, pair, strip(half, 0, start), pr * wr - pi * wi)
                put_split(0, pair, strip(half, 1, start), pr * wi + pi * wr)

    def right_product(stage, pair, table):
        high, low = table
        a, b = operands[stage, 0, pair], operands[stage, 1, pair]
        value = dot(a, high[...]) + dot(b, high[...]) + dot(a, low[...])
        for half in range(2):
            for part in range(2):
                for start in range(0, M, CHUNK):
                    piece = value[half * M + start : half * M + start + CHUNK, part * M : (part + 1) * M]
                    put_split(stage + 1, pair, strip(part, half, start), piece)

    def left_product(stage, pair, table):
        high, low = table
        a, b = operands[stage, 0, pair], operands[stage, 1, pair]
        return dot(high[...], a) + dot(high[...], b) + dot(low[...], a)

    def first_right(step, pair):
        right_product(0, pair, forward)

    def first_left(step, pair):
        far = left_product(1, pair, backward)
        for half in range(2):
            number = data_list[step * BATCH + 2 * pair + half]
            for start in range(0, M, CHUNK):
                fr = far[start : start + CHUNK, half * M : (half + 1) * M]
                fi = far[M + start : M + start + CHUNK, half * M : (half + 1) * M]
                measured = data[number, pl.ds(start, CHUNK), :]
                ratio = 1.0 - measured / (fr * fr + fi * fi + offset_level)
                put_split(2, pair, strip(half, 0, start), fr * ratio)
                put_split(2, pair, strip(half, 1, start), fi * ratio)

    def second_right(step, pair):
        right_product(2, pair, backward)

    def second_left(step, pair):
        back = left_product(3, pair, forward)
        for half in range(2):
            index = 2 * pair + half
            _, row, block, turn, lane = place(step, index)
            back_lanes = (LANES - lane) & (LANES - 1)
            later = lane_of_chunk >= lane
            kept = row_of_tile >= turn
            kept_at = lax.rem(step, 2) * BATCH + index
            for start in range(0, M, CHUNK):
                rows_now = pl.ds(start, CHUNK)
                cr = back[start : start + CHUNK, half * M : (half + 1) * M]
                ci = back[M + start : M + start + CHUNK, half * M : (half + 1) * M]
                wr, wi = window[kept_at, 0, rows_now, :], window[kept_at, 1, rows_now, :]
                pr, pi = framed[kept_at, 0, rows_now, :], framed[kept_at, 1, rows_now, :]
                terms = (wr * cr + wi * ci, wr * ci - wi * cr, wr * wr + wi * wi)
                places, values = [], []
                for kind, term in enumerate(terms):
                    places.append((turn, kind, rows_now, slice(None)))
                    values.append(turned_sums[turn, kind, rows_now, :] + pltpu.roll(term, back_lanes, 1))
                for at, value in zip(places, values):
                    turned_sums[at] = value
                terms = (pr * cr + pi * ci, pr * ci - pi * cr, pr * pr + pi * pi)
                places, values = [], []
                for kind, term in enumerate(terms):
                    for beside in range(2):
                        piece = jnp.where(later, 0.0, term) if beside else jnp.where(later, term, 0.0)
                        if start == 0:
                            top = piece[:8]
                            piece = jnp.concatenate([jnp.where(kept, top, 0.0), piece[8:]], axis=0)
                            at = (kind, block + beside, pl.ds(pl.multiple_of(row + M, 8), 8), slice(None))
                            places.append(at)
                            values.append(sums_ref[at] + jnp.where(kept, 0.0, top))
                        at = (kind, block + beside, pl.ds(pl.multiple_of(row + start, 8), CHUNK), slice(None))
                        places.append(at)
                        values.append(sums_ref[at] + piece)
                for at, value in zip(places, values):
                    sums_ref[at] = value

    batches = jnp.maximum(lax.div(total + (BATCH - 1), BATCH), 1)
    pairs = range(BATCH // 2)

    def run(order, step):
        for phase, back in order:
            for pair in pairs:
                phase(step - back, pair)

    def one_batch(step, carry):
        for phase, back, pair in both_halves:
            phase(step - back, pair)
        return carry

    both_halves = ((second_right, 1, 0), (load, 0, 0), (second_right, 1, 1), (first_right, 0, 0), (load, 0, 1), (second_left, 1, 0), (first_right, 0, 1), (second_left, 1, 1), (first_left, 0, 0), (first_left, 0, 1))
    run(((load, 0), (first_right, 0), (first_left, 0)), jnp.int32(0))
    lax.fori_loop(1, batches, one_batch, 0)
    run(((second_right, 1), (second_left, 1)), batches)

    for kind in range(3):
        total_of_kind = turned_sums[0, kind]
        for turn in range(1, 8):
            total_of_kind = total_of_kind + pltpu.roll(turned_sums[turn, kind], M - turn, 0)
        probe_sums_ref[kind] = total_of_kind

    half = rows // 2
    for pack, out, block in ((pack_left, left_ref, 0), (pack_right, right_ref, 1 + blocks)):
        def rim(kind, start, length):
            return sums_ref[kind, block, start : start + length, :]

        out[:rows, :] = pack(rim(0, RIM, rows), rim(1, RIM, rows), rows)
        out[rows : rows + half, :] = pack(rim(2, RIM, half), rim(2, RIM + half, half), half)
        at = rows + half
        for start in (0, RIM + rows):
            out[at : at + RIM, :] = pack(rim(0, start, RIM), rim(1, start, RIM), RIM)
            out[at + RIM : at + RIM + RIM // 2, :] = pack(
                rim(2, start, RIM // 2), rim(2, start + RIM // 2, RIM // 2), RIM // 2
            )
            at += RIM + RIM // 2


def patterns(owners, positions, counts, tags, data, field, shifted, tables, sums):
    rows = sums.shape[2] - 2 * RIM
    packed = rows + rows // 2 + 3 * RIM
    entries = data.shape[0] + BATCH
    return pl.pallas_call(
        patterns_kernel,
        out_shape=(
            jax.ShapeDtypeStruct(sums.shape, F32),
            jax.ShapeDtypeStruct((packed, LANES), F32),
            jax.ShapeDtypeStruct((packed, LANES), F32),
            jax.ShapeDtypeStruct((3, M, M), F32),
        ),
        in_specs=[in_smem()] * 4 + [in_vmem()] * 5,
        out_specs=(in_vmem(),) * 4,
        scratch_shapes=[
            pltpu.VMEM((8, 3, M, M), F32),
            pltpu.VMEM((2 * BATCH, 2, M, M), F32),
            pltpu.VMEM((2 * BATCH, 2, M, M), F32),
            pltpu.VMEM((4, 2, BATCH // 2, 2 * M, 2 * M), BF16),
            pltpu.SMEM((entries,), I32),
            pltpu.SMEM((entries,), I32),
            pltpu.SMEM((entries,), I32),
        ],
        input_output_aliases={8: 0},
        compiler_params=pltpu.CompilerParams(
            vmem_limit_bytes=16 << 20
        ),
        name="patterns",
    )(owners, positions, counts, tags, data, field, shifted, tables, sums)


def gather_kernel(
    sums_ref,
    left_ref,
    right_ref,
    probe_sums_ref,
    probe_ref,
    field_ref,
    object_out,
    probe_out,
    lines,
    sides,
    corners,
    across,
    along,
    partial,
    send_sem,
    recv_sem,
):
    blocks = sums_ref.shape[1] - PADDED_BLOCKS - SPARE_BLOCKS
    rows = sums_ref.shape[2] - 2 * RIM
    half = rows // 2
    n_ty, n_tx = lax.axis_size("ty"), lax.axis_size("tx")
    ty, tx = lax.axis_index("ty"), lax.axis_index("tx")
    strip = M // n_tx
    mine = pl.ds(pl.multiple_of(tx * strip, strip), strip)

    def at(down, right):
        return lax.rem(ty + down, n_ty), lax.rem(tx + right, n_tx)

    peers = [at(0, j) for j in range(1, n_tx)] + [at(j, 0) for j in range(1, n_ty)]
    peers += [neighbour(down, right) for down, right in CORNERS]
    barrier = pltpu.get_barrier_semaphore()
    for peer in peers:
        pl.semaphore_signal(barrier, inc=1, device_id=peer, device_id_type=MESH_ID)
    pl.semaphore_wait(barrier, len(peers))

    started = [0]

    def send(source, target, peer):
        slot = started[0]
        started[0] += 1
        copy = pltpu.make_async_remote_copy(
            src_ref=source,
            dst_ref=target,
            send_sem=send_sem.at[slot],
            recv_sem=recv_sem.at[slot],
            device_id=peer,
            device_id_type=MESH_ID,
        )
        copy.start()
        return copy

    first = []
    for j in range(1, n_tx):
        peer = at(0, j)
        there = pl.ds(pl.multiple_of(peer[1] * strip, strip), strip)
        first.append(send(probe_sums_ref.at[:, there, :], across.at[j], peer))
    main = rows + half
    corner = RIM + RIM // 2
    inner = pl.ds(1, blocks)
    fields, lights = pl.ds(0, rows), pl.ds(rows, half)
    rims = [
        send(right_ref.at[fields], sides.at[0, fields], neighbour(0, 1)),
        send(left_ref.at[fields], sides.at[1, fields], neighbour(0, -1)),
        send(sums_ref.at[:, inner, pl.ds(RIM + rows, RIM), :], lines.at[0], neighbour(1, 0)),
        send(sums_ref.at[:, inner, pl.ds(0, RIM), :], lines.at[1], neighbour(-1, 0)),
    ]
    for number, (down, right) in enumerate(CORNERS):
        packed = left_ref if right == -1 else right_ref
        start = main + (0 if down == -1 else corner)
        rims.append(send(packed.at[pl.ds(start, corner)], corners.at[number], neighbour(down, right)))

    def rolled(value):
        return pltpu.roll(value, RIM, 1)

    def finish(block, start, length, totals):
        here = pl.ds(start, length)
        lit = 1.0 / (totals[2] + floor_level)
        for part in range(2):
            old = field_ref[part, 1 + block, pl.ds(start + RIM, length), :]
            object_out[part, here, block * LANES : (block + 1) * LANES] = old - totals[part] * lit

    def own(block, start, length):
        return [sums_ref[kind, 1 + block, pl.ds(start + RIM, length), :] for kind in range(3)]

    def side(block, start, length, late):
        index, right = (0, -1) if block == 0 else (1, 1)
        low = lane_ids(length) < RIM
        lanes = (low if block == 0 else jnp.logical_not(low)) & is_inside(0, right)
        there = sides[index, pl.ds(start, length), :]
        light = sides[index, pl.ds(start + (rows - half if late else rows), length), :]
        values = (there, rolled(there), rolled(light) if late else light)
        return [jnp.where(lanes, value, 0.0) for value in values]

    def plus(a, b):
        return [x + y for x, y in zip(a, b)]

    chunk = RIM

    def middle(step, carry):
        start = pl.multiple_of(step * chunk, chunk)
        for block in range(1, blocks - 1):
            finish(block, start, chunk, own(block, start, chunk))
        return carry

    lax.fori_loop(1, rows // chunk - 1, middle, 0)

    total = probe_sums_ref[:, mine, :]
    for j in range(1, n_tx):
        first[j - 1].wait_recv()
        total = total + across[j]
    partial[...] = total
    second = [send(partial, along.at[j], at(j, 0)) for j in range(1, n_ty)]
    for j in range(1, n_ty):
        second[j - 1].wait_recv()
        total = total + along[j]
    weight = total[2] + tiny_level
    for part in range(2):
        probe_out[part, mine, :] = probe_ref[part, mine, :] - total[part] / weight
    third = [send(probe_out.at[:, mine, :], probe_out.at[:, mine, :], at(0, j)) for j in range(1, n_tx)]
    rims.append(send(right_ref.at[lights], sides.at[0, lights], neighbour(0, 1)))
    rims.append(send(left_ref.at[lights], sides.at[1, lights], neighbour(0, -1)))

    for copy in rims:
        copy.wait_recv()
    for late in (False, True):

        def outer(step, carry):
            start = pl.multiple_of(step * chunk, chunk)
            for block in (0, blocks - 1):
                finish(block, start, chunk, plus(own(block, start, chunk), side(block, start, chunk, late)))
            return carry

        middle_step = half // chunk
        lax.fori_loop(*((middle_step, rows // chunk - 1) if late else (1, middle_step)), outer, 0)
    for line, down in enumerate((-1, 1)):
        start = 0 if down == -1 else rows - RIM
        for block in range(blocks):
            totals = own(block, start, RIM)
            arrived = [jnp.where(is_inside(down, 0), lines[line, kind, block], 0.0) for kind in range(3)]
            totals = plus(totals, arrived)
            if block in (0, blocks - 1):
                totals = plus(totals, side(block, start, RIM, down == 1))
                right = -1 if block == 0 else 1
                number = CORNERS.index((-down, -right))
                low = lane_ids(RIM) < RIM
                lanes = (low if block == 0 else jnp.logical_not(low)) & is_inside(down, right)
                there = corners[number, :RIM, :]
                light = corners[number, RIM:, :]
                values = (there, rolled(there), jnp.concatenate([light, rolled(light)], axis=0))
                totals = plus(totals, [jnp.where(lanes, value, 0.0) for value in values])
            finish(block, start, RIM, totals)

    for copy in first + second + rims:
        copy.wait_send()
    for copy in third:
        copy.wait()


def gather(sums, left, right, probe_sums, probe, field, n_ty, n_tx):
    blocks = sums.shape[1] - PADDED_BLOCKS - SPARE_BLOCKS
    rows = sums.shape[2] - 2 * RIM
    main = rows + rows // 2
    strip = M // n_tx
    copies = 2 * (n_tx - 1) + (n_ty - 1) + 6 + len(CORNERS)
    return pl.pallas_call(
        gather_kernel,
        out_shape=(
            jax.ShapeDtypeStruct((2, rows, blocks * LANES), F32),
            jax.ShapeDtypeStruct((2, M, M), F32),
        ),
        in_specs=[in_vmem()] * 6,
        out_specs=(in_vmem(),) * 2,
        scratch_shapes=[
            pltpu.VMEM((2, 3, blocks, RIM, LANES), F32),
            pltpu.VMEM((2, main, LANES), F32),
            pltpu.VMEM((len(CORNERS), RIM + RIM // 2, LANES), F32),
            pltpu.VMEM((n_tx, 3, strip, M), F32),
            pltpu.VMEM((n_ty, 3, strip, M), F32),
            pltpu.VMEM((3, strip, M), F32),
            pltpu.SemaphoreType.DMA((copies,)),
            pltpu.SemaphoreType.DMA((copies,)),
        ],
        compiler_params=pltpu.CompilerParams(
            collective_id=1, has_side_effects=True, vmem_limit_bytes=12 << 20
        ),
        name="gather",
    )(sums, left, right, probe_sums, probe, field)


def store_kernel(object_ref, probe_ref, object_out, probe_out, sem):
    copies = [
        pltpu.make_async_copy(object_ref, object_out, sem.at[0]),
        pltpu.make_async_copy(probe_ref, probe_out, sem.at[1]),
    ]
    for copy in copies:
        copy.start()
    for copy in copies:
        copy.wait()


def store(new_object, new_probe):
    return pl.pallas_call(
        store_kernel,
        out_shape=(
            jax.ShapeDtypeStruct(new_object.shape, F32),
            jax.ShapeDtypeStruct(new_probe.shape, F32),
        ),
        in_specs=[in_vmem()] * 2,
        out_specs=(in_hbm(),) * 2,
        scratch_shapes=[pltpu.SemaphoreType.DMA((2,))],
        compiler_params=pltpu.CompilerParams(vmem_limit_bytes=8 << 20),
        name="store",
    )(new_object, new_probe)


def solution(mesh):
    n_ty, n_tx = mesh.shape["ty"], mesh.shape["tx"]

    def shards(measured, positions, owners, counts, object_field, probe_field):
        positions, owners = kept_in_hbm(positions[0, 0].T), kept_in_hbm(owners)
        field, data, tags, shifted, tables, sums = spread(
            owners, positions, counts, measured[0, 0], object_field, probe_field
        )
        sums, left, right, probe_sums = patterns(
            owners, positions, counts, tags, data, field, shifted, tables, sums
        )
        return store(*gather(sums, left, right, probe_sums, probe_field, field, n_ty, n_tx))

    placed = (
        P("ty", "tx", None, None, None),
        P("ty", "tx", None, None),
        P("ty", "tx", None),
        P("ty", "tx"),
        P(None, "ty", "tx"),
        P(),
    )
    return jax.shard_map(
        shards, mesh=mesh, in_specs=placed, out_specs=(P(None, "ty", "tx"), P()), check_vma=False
    )
```
